512 devices in a mesh: dp: 16 (over z_lo, core), block: 32 (over y, z_hi, x).
Axes of the slice: x: 4, y: 4, z: 16 (z_hi: 2, z_lo: 8; z = z_hi * 8 + z_lo), core: 2. Of those that a mesh axis runs over, the one named last changes fastest.
Arguments:
- tokens: bfloat16 [4096, 16384], P('dp', 'block'), may hold values from -6 to 6
- upper_left: bfloat16 [64, 256, 1024], P('block', 'dp'), may hold values from -0.375 to 0.375
- upper_right: bfloat16 [256, 256, 256], P('block', 'dp'), may hold values from -0.375 to 0.375
- lower_right: bfloat16 [256, 256, 256], P('block', 'dp'), may hold values from -0.375 to 0.375
- lower_left: bfloat16 [64, 1024, 256], P('block', 'dp'), may hold values from -0.1875 to 0.1875
- cotangent: bfloat16 [4096, 16384], P('dp', 'block'), may hold values from -6 to 6
Outputs:
- output: bfloat16 [4096, 16384], P('dp', 'block')
- token_grad: bfloat16 [4096, 16384], P('dp', 'block')
- upper_left_grad: float32 [64, 256, 1024], P('block', 'dp')
- upper_right_grad: float32 [256, 256, 256], P('block', 'dp')
- lower_right_grad: float32 [256, 256, 256], P('block', 'dp')
- lower_left_grad: float32 [64, 1024, 256], P('block', 'dp')
The draws below stay inside these ranges and needn't reach their ends.
All inputs are finite; a program needn't handle non-finite values.
Results may differ from the reference program's by a relative error of at most 0.017.
Values may be sent and summed in bfloat16 or wider, within the bound.
A program may use at most 64 MiB of HBM per device.

```python
import jax
import jax.numpy as jnp
from jax import lax

D = 16384
H = 65536
B = 256
TOK_DEV = 256
E = 4
NB = 64
TOKENS = 4096
N_DP = 16


def level_of(own_key, dims, shards, smallest, top_value):
    loudness, own = 1.0, jax.random.fold_in(own_key, 6)
    for dim, shards_of in shards:
        heights = jnp.exp(jax.random.uniform(jax.random.fold_in(own, dim), (shards_of,), jnp.float32, smallest / len(shards), top_value / len(shards)))
        loudness = loudness * jnp.repeat(heights, dims[dim] // shards_of).reshape([-1 if axis == dim else 1 for axis in range(len(dims))])
    return loudness


def bell_draw(own_key, extent, spread, limit, split=(), held_as=jnp.bfloat16):
    gain = level_of(own_key, extent, split, -0.22, 0.18) if split else 1.0
    entries = jax.random.normal(own_key, extent, jnp.float32) * spread * gain
    return jnp.minimum(jnp.maximum(entries, -limit), limit).astype(held_as)


def setup_inputs(seed: int = 0) -> dict:
    splits = jax.random.split(jax.random.key(seed), 7)
    return {
        "tokens": bell_draw(splits[0], (TOKENS, D), 1.0, 6.0, ((0, 16), (1, 32))),
        "upper_left": bell_draw(splits[1], (NB, B, E * B), B ** -0.5, 0.375, ((0, 32), (1, 16))),
        "upper_right": bell_draw(splits[2], (B, B, B), B ** -0.5, 0.375, ((0, 32), (1, 16))),
        "lower_right": bell_draw(splits[3], (B, B, B), B ** -0.5, 0.375, ((0, 32), (1, 16))),
        "lower_left": bell_draw(splits[4], (NB, E * B, B), (E * B) ** -0.5, 0.1875, ((0, 32), (1, 16))),
        "cotangent": bell_draw(splits[5], (TOKENS, D), 1.0, 6.0, ((0, 16), (1, 32))),
    }


def product(form, left, right):
    return jnp.einsum(form, left.astype(jnp.float32), right.astype(jnp.float32), precision=lax.Precision.HIGHEST)

def shard_pass(carry, pair):
    tokens_part, cot_part, upper_left, upper_right, lower_right, lower_left = pair
    rows = tokens_part.shape[0]
    expand = H // D
    blocks = D // B
    x_three = tokens_part.reshape(rows, blocks, B)
    left_four = upper_left.reshape(blocks, B, expand, B)
    mixed = product('tkb,kbec->kect', x_three, left_four).astype(jnp.bfloat16).reshape(B, B, rows)
    hidden_pre = product('act,cab->cbt', mixed, upper_right)
    active = jax.nn.gelu(hidden_pre).astype(jnp.bfloat16)
    narrow = product('cbt,cbe->cet', active, lower_right).astype(jnp.bfloat16)
    narrow_four = narrow.reshape(B, blocks, expand, rows)
    out_four = lower_left.reshape(blocks, expand, B, B)
    result = product('ckft,kfco->tko', narrow_four, out_four).astype(jnp.bfloat16).reshape(rows, D)
    cot_three = cot_part.reshape(rows, blocks, B)
    grad_lower_left = product('ckft,tko->kfco', narrow_four, cot_three).reshape(blocks, expand * B, B)
    back_narrow = product('tko,kfco->kfct', cot_three, out_four).astype(jnp.bfloat16).reshape(B, B, rows)
    grad_lower_right = product('cbt,ect->cbe', active, back_narrow)
    back_active = product('ect,cbe->cbt', back_narrow, lower_right)
    back_pre = jax.vjp(jax.nn.gelu, hidden_pre)[1](back_active)[0].astype(jnp.bfloat16)
    grad_upper_right = product('act,cbt->cab', mixed, back_pre)
    back_mixed = product('cbt,cab->cat', back_pre, upper_right).astype(jnp.bfloat16).reshape(B, blocks, expand, rows)
    grad_upper_left = product('tkb,cket->kbec', x_three, back_mixed).reshape(blocks, B, expand * B)
    token_grad = product('cket,kbec->tkb', back_mixed, left_four).astype(jnp.bfloat16).reshape(rows, D)
    parts = (grad_upper_left, grad_upper_right, grad_lower_right, grad_lower_left)
    carry = tuple((total + part.astype(jnp.bfloat16).astype(jnp.float32) for total, part in zip(carry, parts)))
    return (carry, (result, token_grad))

def reference(tokens, upper_left, upper_right, lower_right, lower_left, cotangent):
    tokens_split = tokens.reshape(N_DP, TOK_DEV, D)
    cot_split = cotangent.reshape(N_DP, TOK_DEV, D)
    start = (jnp.zeros(upper_left.shape, jnp.float32), jnp.zeros(upper_right.shape, jnp.float32), jnp.zeros(lower_right.shape, jnp.float32), jnp.zeros(lower_left.shape, jnp.float32))

    def step(carry, pair):
        return shard_pass(carry, (pair[0], pair[1], upper_left, upper_right, lower_right, lower_left))
    totals, stacked = lax.scan(step, start, (tokens_split, cot_split))
    output = stacked[0].reshape(TOKENS, D)
    token_grad = stacked[1].reshape(TOKENS, D)
    return (output, token_grad, totals[0], totals[1], totals[2], totals[3])
```

```python
import functools

import jax
import jax.numpy as jnp
from jax import lax
from jax.experimental import pallas as pl
from jax.experimental.pallas import tpu as pltpu
from jax.sharding import PartitionSpec as P

ZL, CORES, NY, ZH, NX = 8, 2, 4, 2, 4
RING = ZL * ZH
BF = jnp.bfloat16
F32 = jnp.float32


def contract(form, left, right):
    return jnp.einsum(form, left, right, preferred_element_type=F32)


def place():
    dp = lax.axis_index("dp")
    block = lax.axis_index("block")
    zl, core = dp // CORES, dp % CORES
    y, rest = block // (ZH * NX), block % (ZH * NX)
    zh, x = rest // NX, rest % NX
    return zl, core, y, zh, x


def at(z, core, y, x):
    z = z % RING
    return {
        "dp": (z % ZL) * CORES + core,
        "block": y * (ZH * NX) + (z // ZL) * NX + x,
    }


def greet(z, core, y, x):
    barrier = pltpu.get_barrier_semaphore()
    for who in (at(z + 1, core, y, x), at(z + RING - 1, core, y, x), at(z, 1 - core, y, x)):
        pl.semaphore_signal(barrier, inc=1, device_id=who, device_id_type=pl.DeviceIdType.MESH)
    pl.semaphore_wait(barrier, 3)


def gather_kernel(count, *refs):
    own, out = refs[:count], refs[count : 2 * count]
    send, recv, local = refs[2 * count :]
    zl, core, y, zh, x = place()
    z = zh * ZL + zl
    right, left = at(z + 1, core, y, x), at(z + RING - 1, core, y, x)
    other = at(z, 1 - core, y, x)
    greet(z, core, y, x)

    def spot(w, source):
        source = source % RING
        return out[w].at[source // ZL, :, source % ZL, core]

    def push(w, slot, source, target, src=None):
        where = spot(w, source)
        copy = pltpu.make_async_remote_copy(
            src_ref=where if src is None else src,
            dst_ref=where,
            send_sem=send.at[w, slot],
            recv_sem=recv.at[w, slot],
            device_id=target,
            device_id_type=pl.DeviceIdType.MESH,
        )
        copy.start()
        return copy

    half = RING // 2
    sent = []
    rights, lefts, keeps = [], [], []
    for w in range(count):
        src = own[w]
        rights.append(push(w, 0, z, right, src))
        lefts.append(push(w, half, z, left, src))
        sent.append(push(w, RING - 1, z, other, src))
        keep = pltpu.make_async_copy(src, spot(w, z), local.at[w])
        keep.start()
        keeps.append(keep)
    for s in range(1, half + 1):
        for w in range(count):
            rights[w].wait_recv()
            sent.append(rights[w])
            if s < half:
                rights[w] = push(w, s, z + RING - s, right)
            sent.append(push(w, RING + s, z + RING - s, other))
            if s < half:
                lefts[w].wait_recv()
                sent.append(lefts[w])
                if s < half - 1:
                    lefts[w] = push(w, half + s, z + s, left)
                sent.append(push(w, RING + half + s, z + s, other))
    mirrors = [
        (w, slot)
        for w in range(count)
        for slot in [RING - 1] + list(range(RING + 1, RING + half + half))
    ]
    for w, slot in mirrors:
        pltpu.make_async_remote_copy(
            src_ref=own[w],
            dst_ref=own[w],
            send_sem=send.at[w, slot],
            recv_sem=recv.at[w, slot],
            device_id=other,
            device_id_type=pl.DeviceIdType.MESH,
        ).wait_recv()
    for copy in sent:
        copy.wait_send()
    for keep in keeps:
        keep.wait()


def ring_gather(shards, collective_id):
    count = len(shards)
    slots = 2 * RING
    shapes = [
        jax.ShapeDtypeStruct((ZH, s.shape[0], ZL, CORES) + s.shape[1:], s.dtype) for s in shards
    ]
    outs = pl.pallas_call(
        functools.partial(gather_kernel, count),
        out_shape=shapes,
        in_specs=[pl.BlockSpec(memory_space=pltpu.VMEM)] * count,
        out_specs=[pl.BlockSpec(memory_space=pl.ANY)] * count,
        scratch_shapes=[
            pltpu.SemaphoreType.DMA((count, slots)),
            pltpu.SemaphoreType.DMA((count, slots)),
            pltpu.SemaphoreType.DMA((count,)),
        ],
        compiler_params=pltpu.CompilerParams(collective_id=collective_id, has_side_effects=True),
        name="ring_gather",
    )(*shards)
    return [
        o.reshape(ZH * s.shape[0], ZL * CORES * s.shape[1], s.shape[2])
        for o, s in zip(outs, shards)
    ]


def scatter_kernel(count, *refs):
    part, out = refs[:count], refs[count : 2 * count]
    rest = refs[2 * count :]
    mate, come, stage = rest[:count], rest[count : 2 * count], rest[2 * count : 3 * count]
    send, recv, msend, mrecv = rest[3 * count :]
    zl, core, y, zh, x = place()
    z = zh * ZL + zl
    right, left = at(z + 1, core, y, x), at(z + RING - 1, core, y, x)
    other = at(z, 1 - core, y, x)
    greet(z, core, y, x)
    half = RING // 2

    def goal(slot):
        if slot < half:
            return (z + half - slot) % RING
        return (z + RING - (half - 1) + (slot - half)) % RING

    order = []
    for s in range(half):
        order.append(s)
        if half + s < RING - 1:
            order.append(half + s)
    order.append(RING - 1)

    mates = {}
    for slot in order:
        d = goal(slot)
        for w in range(count):
            copy = pltpu.make_async_remote_copy(
                src_ref=part[w].at[d // ZL, :, d % ZL, 1 - core],
                dst_ref=mate[w].at[slot],
                send_sem=msend.at[w, slot],
                recv_sem=mrecv.at[w, slot],
                device_id=other,
                device_id_type=pl.DeviceIdType.MESH,
            )
            copy.start()
            mates[w, slot] = copy
    moves = {}
    for slot in order:
        d = goal(slot)
        for w in range(count):
            mates[w, slot].wait_recv()
            total = part[w][d // ZL, :, d % ZL, core].astype(F32) + mate[w][slot].astype(F32)
            if slot == RING - 1:
                for last in (half - 1, RING - 2):
                    moves[w, last].wait_recv()
                    total = total + come[w][last].astype(F32)
                out[w][...] = total
                continue
            if slot not in (0, half):
                moves[w, slot - 1].wait_recv()
                total = total + come[w][slot - 1].astype(F32)
            stage[w][slot] = total.astype(BF)
            copy = pltpu.make_async_remote_copy(
                src_ref=stage[w].at[slot],
                dst_ref=come[w].at[slot],
                send_sem=send.at[w, slot],
                recv_sem=recv.at[w, slot],
                device_id=right if slot < half else left,
                device_id_type=pl.DeviceIdType.MESH,
            )
            copy.start()
            moves[w, slot] = copy
    for copy in mates.values():
        copy.wait_send()
    for copy in moves.values():
        copy.wait_send()


def ring_scatter(parts, collective_id):
    count = len(parts)
    split, shards = [], []
    for p in parts:
        shard = (p.shape[0] // ZH, p.shape[1] // (ZL * CORES), p.shape[2])
        shards.append(shard)
        split.append(p.reshape(ZH, shard[0], ZL, CORES, shard[1], shard[2]))
    return pl.pallas_call(
        functools.partial(scatter_kernel, count),
        out_shape=[jax.ShapeDtypeStruct(s, F32) for s in shards],
        in_specs=[pl.BlockSpec(memory_space=pltpu.VMEM)] * count,
        out_specs=[pl.BlockSpec(memory_space=pltpu.VMEM)] * count,
        scratch_shapes=[pltpu.VMEM((RING,) + s, BF) for s in shards]
        + [pltpu.VMEM((RING - 1,) + s, BF) for s in shards]
        + [pltpu.VMEM((RING - 1,) + s, BF) for s in shards]
        + [
            pltpu.SemaphoreType.DMA((count, RING - 1)),
            pltpu.SemaphoreType.DMA((count, RING - 1)),
            pltpu.SemaphoreType.DMA((count, RING)),
            pltpu.SemaphoreType.DMA((count, RING)),
        ],
        compiler_params=pltpu.CompilerParams(
            collective_id=collective_id, has_side_effects=True, vmem_limit_bytes=56 * 2**20
        ),
        name="ring_scatter",
    )(*split)


GROUPS = [
    [y * (ZH * NX) + zh * NX + x for y in range(NY) for x in range(NX)] for zh in range(ZH)
]
SWAP = [(b, b ^ NX) for b in range(NY * ZH * NX)]


def exchange(values):
    return lax.all_to_all(
        values, "block", split_axis=0, concat_axis=0, tiled=True, axis_index_groups=GROUPS
    )


def to_columns(values):
    n, k, e, c, t = values.shape
    cols = c // (NY * ZH * NX)
    kl = k // ZH
    v = values.reshape(n, k * e, NY, ZH, NX, cols, t)
    v = v.transpose(2, 4, 0, 3, 5, 1, 6).reshape(NY * NX, n, ZH * cols, k * e, t)
    v = exchange(v)
    v = v.reshape(NY, NX, n, ZH * cols, ZH, kl * e, t)
    return v.transpose(2, 3, 0, 4, 1, 5, 6).reshape(n, ZH * cols, NY * NX * k * e, t)


def to_rows(values, kl):
    n, c, a, t = values.shape
    rows = a // (NY * ZH * NX)
    cols = c // ZH
    v = values.reshape(n, c, NY, ZH, NX, rows, t)
    v = v.transpose(2, 4, 0, 3, 5, 1, 6).reshape(NY * NX, n, ZH * rows, c, t)
    v = exchange(v)
    v = v.reshape(NY, NX, n, ZH * rows, ZH, cols, t)
    v = v.transpose(2, 3, 0, 4, 1, 5, 6)
    return v.reshape(n, ZH * kl, rows // kl, NY * NX * c, t)


def local(tokens, upper_left, upper_right, lower_right, lower_left, cotangent):
    zl, core, y, zh, x = place()
    rows, features = tokens.shape
    width = upper_left.shape[1] * ZL * CORES
    kl = upper_left.shape[0]
    expand = upper_left.shape[2] // width
    few = rows // ZH
    low = zh == 0

    both = jnp.stack([tokens, cotangent]).reshape(2, ZH, few, features)
    mine = jnp.where(low, both[:, 0], both[:, 1])
    away = jnp.where(low, both[:, 1], both[:, 0])
    came = lax.ppermute(away, "block", SWAP)
    pair = jnp.stack([jnp.where(low, mine, came), jnp.where(low, came, mine)], axis=2)
    pair = pair.reshape(2, few, ZH * kl, width)
    toks, cots = pair[0], pair[1]

    in_left, out_left, in_right, out_right = ring_gather(
        (upper_left, lower_left, upper_right, lower_right), 1
    )
    left_four = in_left.reshape(ZH * kl, width, expand, width)
    out_four = out_left.reshape(ZH * kl, expand, width, width)

    mixed = contract("tkb,kbec->kect", toks, left_four).astype(BF)
    back_narrow = contract("tko,kfco->kfct", cots, out_four).astype(BF)
    columns = to_columns(jnp.stack([mixed, back_narrow]))
    spread, narrow_back = columns[0], columns[1]

    hidden_pre = contract("cat,cab->cbt", spread, in_right)
    active = jax.nn.gelu(hidden_pre).astype(BF)
    narrow = contract("cbt,cbe->cet", active, out_right).astype(BF)
    back_active = contract("cet,cbe->cbt", narrow_back, out_right)
    back_pre = jax.vjp(jax.nn.gelu, hidden_pre)[1](back_active)[0].astype(BF)
    back_mixed = contract("cbt,cab->cat", back_pre, in_right).astype(BF)
    rowed = to_rows(jnp.stack([narrow, back_mixed]), kl)
    narrow_four, mixed_back = rowed[0], rowed[1]

    grad_lower_right = contract("cbt,cet->cbe", active, narrow_back).astype(BF)
    grad_upper_right = contract("cat,cbt->cab", spread, back_pre).astype(BF)
    result = contract("kfct,kfco->tko", narrow_four, out_four).astype(BF)
    token_grad = contract("kect,kbec->tkb", mixed_back, left_four).astype(BF)

    ends = jnp.stack([result, token_grad]).reshape(2, few, ZH, features)
    keep = jnp.where(low, ends[:, :, 0], ends[:, :, 1])
    away = jnp.where(low, ends[:, :, 1], ends[:, :, 0])
    came = lax.ppermute(away, "block", SWAP)
    ends = jnp.concatenate([jnp.where(low, keep, came), jnp.where(low, came, keep)], axis=1)

    grad_lower_left = contract("kfct,tko->kfco", narrow_four, cots).astype(BF)
    grad_upper_left = contract("tkb,kect->kbec", toks, mixed_back).astype(BF)
    g_ul, g_ll, g_ur, g_lr = ring_scatter(
        (
            grad_upper_left.reshape(in_left.shape),
            grad_lower_left.reshape(out_left.shape),
            grad_upper_right,
            grad_lower_right,
        ),
        2,
    )
    return ends[0], ends[1], g_ul, g_ur, g_lr, g_ll


def solution(mesh):
    in_specs = (
        P("dp", "block"),
        P("block", "dp", None),
        P("block", "dp", None),
        P("block", "dp", None),
        P("block", "dp", None),
        P("dp", "block"),
    )
    out_specs = (
        P("dp", "block"),
        P("dp", "block"),
        P("block", "dp", None),
        P("block", "dp", None),
        P("block", "dp", None),
        P("block", "dp", None),
    )
    return jax.shard_map(local, mesh=mesh, in_specs=in_specs, out_specs=out_specs, check_vma=False)
```

```python
import functools

import jax
import jax.numpy as jnp
from jax import lax
from jax.experimental import pallas as pl
from jax.experimental.pallas import tpu as pltpu
from jax.sharding import PartitionSpec as P

ZL, CORES, NY, ZH, NX = 8, 2, 4, 2, 4
RING = ZL * ZH
BF = jnp.bfloat16
F32 = jnp.float32


def contract(form, left, right):
    return jnp.einsum(form, left, right, preferred_element_type=F32)


def place():
    dp = lax.axis_index("dp")
    block = lax.axis_index("block")
    zl, core = dp // CORES, dp % CORES
    y, rest = block // (ZH * NX), block % (ZH * NX)
    zh, x = rest // NX, rest % NX
    return zl, core, y, zh, x


def at(z, core, y, x):
    z = z % RING
    return {
        "dp": (z % ZL) * CORES + core,
        "block": y * (ZH * NX) + (z // ZL) * NX + x,
    }


def greet(others):
    barrier = pltpu.get_barrier_semaphore()
    for who in others:
        pl.semaphore_signal(barrier, inc=1, device_id=who, device_id_type=pl.DeviceIdType.MESH)
    pl.semaphore_wait(barrier, len(others))


def remote(src, dst, send, recv, target):
    return pltpu.make_async_remote_copy(
        src_ref=src,
        dst_ref=dst,
        send_sem=send,
        recv_sem=recv,
        device_id=target,
        device_id_type=pl.DeviceIdType.MESH,
    )


class Swap:
    STEPS = (3,)
    WAYS = (RING // 4, RING - RING // 4)

    @staticmethod
    def scratch(arrays):
        shape = arrays[0].shape
        return [
            pltpu.VMEM(shape, BF),
            pltpu.SemaphoreType.DMA((2, 2)),
            pltpu.SemaphoreType.DMA((2, 2)),
        ]

    @staticmethod
    def outs(arrays):
        return [jax.ShapeDtypeStruct(v.shape, v.dtype) for v in arrays]

    def __init__(self, ins, outs, scratch):
        self.src, self.out = ins[0], outs[0]
        self.relay, self.send, self.recv = scratch
        zl, core, y, zh, x = place()
        z = zh * ZL + zl
        self.targets = [at(z + way, core, y, x) for way in self.WAYS]

    def peers(self):
        return self.targets

    def start(self):
        self.first = [
            remote(
                self.src.at[j], self.relay.at[j], self.send.at[0, j], self.recv.at[0, j], who
            )
            for j, who in enumerate(self.targets)
        ]
        for copy in self.first:
            copy.start()

    def step(self, s):
        if s not in self.STEPS:
            return
        self.second = []
        for j, who in enumerate(self.targets):
            self.first[j].wait_recv()
            copy = remote(
                self.relay.at[j], self.out.at[j], self.send.at[1, j], self.recv.at[1, j], who
            )
            copy.start()
            self.second.append(copy)

    def finish(self):
        for copy in self.second:
            copy.wait_recv()
        for copy in self.first + self.second:
            copy.wait_send()


class Spread:
    RELAYS = (
        (0, 2, 0, 1),
        (2, 0, 1, 0),
        (3, 2, 0, 3),
        (2, 1, 3, 0),
        (1, 2, 0, 1),
        (2, 3, 3, 0),
        (2, 2, 0, 3),
    )
    STEPS = {3: (0, 1, 2), 5: (3, 4, 5, 6)}

    @staticmethod
    def scratch(arrays):
        n, hops = len(arrays), len(Spread.RELAYS)
        return [pltpu.VMEM((hops,) + v.shape[1:], BF) for v in arrays] + [
            pltpu.SemaphoreType.DMA((n, NY * NX)),
            pltpu.SemaphoreType.DMA((n, NY * NX)),
            pltpu.SemaphoreType.DMA((n, hops)),
            pltpu.SemaphoreType.DMA((n, hops)),
            pltpu.SemaphoreType.DMA((n,)),
        ]

    @staticmethod
    def outs(arrays):
        return [jax.ShapeDtypeStruct(v.shape, v.dtype) for v in arrays]

    def __init__(self, ins, outs, scratch):
        self.n = len(ins)
        self.src, self.out = ins, outs
        self.relay = scratch[: self.n]
        self.send, self.recv, self.rsend, self.rrecv, self.own = scratch[self.n :]
        zl, self.core, self.y, zh, self.x = place()
        self.z = zh * ZL + zl

    def device(self, dy, dx):
        return at(self.z, self.core, (self.y + dy) % NY, (self.x + dx) % NX)

    def index(self, dy, dx):
        return (self.y + dy) % NY * NX + (self.x + dx) % NX

    def peers(self):
        return [self.device(dy, dx) for dy in range(NY) for dx in range(NX) if dy or dx]

    def start(self):
        me = self.index(0, 0)
        self.sent, self.legs, self.keeps, self.comes = [], {}, [], []
        for j, (dy, dx, ry, rx) in enumerate(self.RELAYS):
            for w in range(self.n):
                copy = remote(
                    self.src[w].at[self.index(dy, dx)],
                    self.relay[w].at[j],
                    self.rsend.at[w, j],
                    self.rrecv.at[w, j],
                    self.device(ry, rx),
                )
                copy.start()
                self.legs[w, j] = copy
        for dy in range(NY):
            for dx in range(NX):
                if not (dy or dx) or 2 in (dy, dx):
                    continue
                for w in range(self.n):
                    copy = remote(
                        self.src[w].at[self.index(dy, dx)],
                        self.out[w].at[me],
                        self.send.at[w, dy * NX + dx],
                        self.recv.at[w, dy * NX + dx],
                        self.device(dy, dx),
                    )
                    copy.start()
                    self.sent.append(copy)
                    self.comes.append(copy)
        for w in range(self.n):
            keep = pltpu.make_async_copy(self.src[w].at[me], self.out[w].at[me], self.own.at[w])
            keep.start()
            self.keeps.append(keep)

    def step(self, s):
        for j in self.STEPS.get(s, ()):
            dy, dx, ry, rx = self.RELAYS[j]
            for w in range(self.n):
                self.legs[w, j].wait_recv()
                self.sent.append(self.legs[w, j])
                copy = remote(
                    self.relay[w].at[j],
                    self.out[w].at[self.index(NY - ry, NX - rx)],
                    self.send.at[w, dy * NX + dx],
                    self.recv.at[w, dy * NX + dx],
                    self.device(dy - ry + NY, dx - rx + NX),
                )
                copy.start()
                self.sent.append(copy)
                self.comes.append(copy)

    def finish(self):
        for copy in self.comes:
            copy.wait_recv()
        for copy in self.sent:
            copy.wait_send()
        for keep in self.keeps:
            keep.wait()


def gather_kernel(count, kind, extra, *refs):
    own, refs = refs[:count], refs[count:]
    side_in, refs = refs[:extra], refs[extra:]
    out, refs = refs[:count], refs[count:]
    side_out, refs = refs[:extra], refs[extra:]
    (send, recv, local), refs = refs[:3], refs[3:]
    side = kind(side_in, side_out, refs)
    zl, core, y, zh, x = place()
    z = zh * ZL + zl
    right, left = at(z + 1, core, y, x), at(z + RING - 1, core, y, x)
    other = at(z, 1 - core, y, x)
    greet([right, left, other] + side.peers())

    def spot(w, source):
        source = source % RING
        return out[w].at[source // ZL, :, source % ZL, core]

    def push(w, slot, source, target, src=None):
        where = spot(w, source)
        copy = remote(
            where if src is None else src, where, send.at[w, slot], recv.at[w, slot], target
        )
        copy.start()
        return copy

    half = RING // 2
    sent = []
    rights, lefts, keeps = [], [], []
    for w in range(count):
        src = own[w]
        rights.append(push(w, 0, z, right, src))
        lefts.append(push(w, half, z, left, src))
    side.start()
    for w in range(count):
        src = own[w]
        sent.append(push(w, RING - 1, z, other, src))
        keep = pltpu.make_async_copy(src, spot(w, z), local.at[w])
        keep.start()
        keeps.append(keep)
    for s in range(1, half + 1):
        for w in range(count):
            rights[w].wait_recv()
            sent.append(rights[w])
            if s < half:
                rights[w] = push(w, s, z + RING - s, right)
            sent.append(push(w, RING + s, z + RING - s, other))
            if s < half:
                lefts[w].wait_recv()
                sent.append(lefts[w])
                if s < half - 1:
                    lefts[w] = push(w, half + s, z + s, left)
                sent.append(push(w, RING + half + s, z + s, other))
        side.step(s)
    side.finish()
    for w in range(count):
        for slot in [RING - 1] + list(range(RING + 1, 2 * RING)):
            remote(own[w], own[w], send.at[w, slot], recv.at[w, slot], other).wait_recv()
    for copy in sent:
        copy.wait_send()
    for keep in keeps:
        keep.wait()


def ring_gather(shards, kind, arrays, collective_id):
    count, extra = len(shards), len(arrays)
    slots = 2 * RING
    shapes = [
        jax.ShapeDtypeStruct((ZH, s.shape[0], ZL, CORES) + s.shape[1:], s.dtype) for s in shards
    ]
    outs = pl.pallas_call(
        functools.partial(gather_kernel, count, kind, extra),
        out_shape=shapes + kind.outs(arrays),
        in_specs=[pl.BlockSpec(memory_space=pltpu.VMEM)] * (count + extra),
        out_specs=[pl.BlockSpec(memory_space=pl.ANY)] * (count + extra),
        scratch_shapes=[
            pltpu.SemaphoreType.DMA((count, slots)),
            pltpu.SemaphoreType.DMA((count, slots)),
            pltpu.SemaphoreType.DMA((count,)),
        ]
        + kind.scratch(arrays),
        compiler_params=pltpu.CompilerParams(collective_id=collective_id, has_side_effects=True),
        name="ring_gather",
    )(*shards, *arrays)
    full = [
        o.reshape(ZH * s.shape[0], ZL * CORES * s.shape[1], s.shape[2])
        for o, s in zip(outs[:count], shards)
    ]
    return full, outs[count:]


def scatter_kernel(count, kind, extra, *refs):
    part, refs = refs[:count], refs[count:]
    side_in, refs = refs[:extra], refs[extra:]
    out, refs = refs[:count], refs[count:]
    side_out, refs = refs[:extra], refs[extra:]
    mate, come, stage = refs[:count], refs[count : 2 * count], refs[2 * count : 3 * count]
    (send, recv, msend, mrecv), refs = refs[3 * count : 3 * count + 4], refs[3 * count + 4 :]
    side = kind(side_in, side_out, refs)
    zl, core, y, zh, x = place()
    z = zh * ZL + zl
    right, left = at(z + 1, core, y, x), at(z + RING - 1, core, y, x)
    other = at(z, 1 - core, y, x)
    greet([right, left, other] + side.peers())
    half = RING // 2

    def goal(slot):
        if slot < half:
            return (z + half - slot) % RING
        return (z + RING - (half - 1) + (slot - half)) % RING

    order = []
    for s in range(half):
        order.append(s)
        if half + s < RING - 1:
            order.append(half + s)
    order.append(RING - 1)

    mates = {}

    def trade(slot):
        d = goal(slot)
        for w in range(count):
            copy = remote(
                part[w].at[d // ZL, :, d % ZL, 1 - core],
                mate[w].at[slot],
                msend.at[w, slot],
                mrecv.at[w, slot],
                other,
            )
            copy.start()
            mates[w, slot] = copy

    for slot in order[:4]:
        trade(slot)
    side.start()
    for slot in order[4:]:
        trade(slot)
    moves = {}
    for slot in order:
        d = goal(slot)
        for w in range(count):
            mates[w, slot].wait_recv()
            total = part[w][d // ZL, :, d % ZL, core].astype(F32) + mate[w][slot].astype(F32)
            if slot == RING - 1:
                for last in (half - 1, RING - 2):
                    moves[w, last].wait_recv()
                    total = total + come[w][last].astype(F32)
                out[w][...] = total
                continue
            if slot not in (0, half):
                moves[w, slot - 1].wait_recv()
                total = total + come[w][slot - 1].astype(F32)
            stage[w][slot] = total.astype(BF)
            copy = remote(
                stage[w].at[slot],
                come[w].at[slot],
                send.at[w, slot],
                recv.at[w, slot],
                right if slot < half else left,
            )
            copy.start()
            moves[w, slot] = copy
        if slot < half:
            side.step(slot)
    side.finish()
    for copy in mates.values():
        copy.wait_send()
    for copy in moves.values():
        copy.wait_send()


def ring_scatter(parts, kind, arrays, collective_id):
    count, extra = len(parts), len(arrays)
    split, shards = [], []
    for p in parts:
        shard = (p.shape[0] // ZH, p.shape[1] // (ZL * CORES), p.shape[2])
        shards.append(shard)
        split.append(p.reshape(ZH, shard[0], ZL, CORES, shard[1], shard[2]))
    outs = pl.pallas_call(
        functools.partial(scatter_kernel, count, kind, extra),
        out_shape=[jax.ShapeDtypeStruct(s, F32) for s in shards] + kind.outs(arrays),
        in_specs=[pl.BlockSpec(memory_space=pltpu.VMEM)] * (count + extra),
        out_specs=[pl.BlockSpec(memory_space=pltpu.VMEM)] * count
        + [pl.BlockSpec(memory_space=pl.ANY)] * extra,
        scratch_shapes=[pltpu.VMEM((RING,) + s, BF) for s in shards]
        + [pltpu.VMEM((RING - 1,) + s, BF) for s in shards]
        + [pltpu.VMEM((RING - 1,) + s, BF) for s in shards]
        + [
            pltpu.SemaphoreType.DMA((count, RING - 1)),
            pltpu.SemaphoreType.DMA((count, RING - 1)),
            pltpu.SemaphoreType.DMA((count, RING)),
            pltpu.SemaphoreType.DMA((count, RING)),
        ]
        + kind.scratch(arrays),
        compiler_params=pltpu.CompilerParams(
            collective_id=collective_id, has_side_effects=True, vmem_limit_bytes=48 * 2**20
        ),
        name="ring_scatter",
    )(*split, *arrays)
    return outs[:count], outs[count:]


def columns_out(v):
    k, e, c, t = v.shape
    cols = c // (NY * ZH * NX)
    v = v.reshape(k * e, NY, ZH, NX, cols, t).transpose(1, 3, 2, 4, 0, 5)
    return v.reshape(NY * NX, ZH * cols, k * e, t)


def columns_in(v):
    peers, c, a, t = v.shape
    v = v.reshape(NY, NX, c, ZH, a // ZH, t).transpose(2, 0, 3, 1, 4, 5)
    return v.reshape(c, peers * a, t)


def rows_out(v):
    c, a, t = v.shape
    rows = a // (NY * ZH * NX)
    v = v.reshape(c, NY, ZH, NX, rows, t).transpose(1, 3, 2, 4, 0, 5)
    return v.reshape(NY * NX, ZH * rows, c, t)


def rows_in(v, k):
    peers, a, c, t = v.shape
    v = v.reshape(NY, NX, a, ZH, c // ZH, t).transpose(2, 0, 3, 1, 4, 5)
    return v.reshape(k, a // k * peers * c, t)


def local(tokens, upper_left, upper_right, lower_right, lower_left, cotangent):
    zl, core, y, zh, x = place()
    rows, features = tokens.shape
    width = upper_left.shape[1] * ZL * CORES
    kl = upper_left.shape[0]
    k4 = ZH * kl
    expand = upper_left.shape[2] // width
    few = rows // ZH
    low = zh == 0

    both = jnp.stack([tokens, cotangent]).reshape(2, ZH, few, kl, width).transpose(0, 1, 3, 2, 4)
    mine = jnp.where(low, both[:, 0], both[:, 1])
    away = jnp.where(low, both[:, 1], both[:, 0])
    (in_left, out_left), (came,) = ring_gather((upper_left, lower_left), Swap, (away,), 1)
    pair = jnp.concatenate(
        [jnp.where(low, mine, came), jnp.where(low, came, mine)], axis=1
    )
    toks, cots = pair[0], pair[1]

    mixed = contract("ktb,kbj->kjt", toks, in_left).astype(BF)
    back_narrow = contract("kto,kjo->kjt", cots, out_left).astype(BF)
    (in_right, out_right), (spread, narrow_back) = ring_gather(
        (upper_right, lower_right),
        Spread,
        (
            columns_out(mixed.reshape(k4, expand, width, few)),
            columns_out(back_narrow.reshape(k4, expand, width, few)),
        ),
        2,
    )
    spread, narrow_back = columns_in(spread), columns_in(narrow_back)

    hidden_pre = contract("cat,cab->cbt", spread, in_right)
    active = jax.nn.gelu(hidden_pre).astype(BF)
    narrow = contract("cbt,cbe->cet", active, out_right).astype(BF)
    back_active = contract("cet,cbe->cbt", narrow_back, out_right)
    back_pre = jax.vjp(jax.nn.gelu, hidden_pre)[1](back_active)[0].astype(BF)
    back_mixed = contract("cbt,cab->cat", back_pre, in_right).astype(BF)
    grad_lower_right = contract("cbt,cet->cbe", active, narrow_back).astype(BF)
    grad_upper_right = contract("cat,cbt->cab", spread, back_pre).astype(BF)
    (g_ur, g_lr), (narrow, back_mixed) = ring_scatter(
        (grad_upper_right, grad_lower_right), Spread, (rows_out(narrow), rows_out(back_mixed)), 3
    )
    narrow, back_mixed = rows_in(narrow, k4), rows_in(back_mixed, k4)

    result = contract("kjt,kjo->kto", narrow, out_left).astype(BF)
    token_grad = contract("kjt,kbj->ktb", back_mixed, in_left).astype(BF)
    grad_lower_left = contract("kjt,kto->kjo", narrow, cots).astype(BF)
    grad_upper_left = contract("ktb,kjt->kbj", toks, back_mixed).astype(BF)

    ends = jnp.stack([result, token_grad]).reshape(2, ZH, kl, few, width)
    keep = jnp.where(low, ends[:, 0], ends[:, 1])
    away = jnp.where(low, ends[:, 1], ends[:, 0])
    (g_ul, g_ll), (came,) = ring_scatter((grad_upper_left, grad_lower_left), Swap, (away,), 4)
    ends = jnp.stack([jnp.where(low, keep, came), jnp.where(low, came, keep)], axis=1)
    ends = ends.transpose(0, 1, 3, 2, 4).reshape(2, rows, features)
    return ends[0], ends[1], g_ul, g_ur, g_lr, g_ll


def solution(mesh):
    in_specs = (
        P("dp", "block"),
        P("block", "dp", None),
        P("block", "dp", None),
        P("block", "dp", None),
        P("block", "dp", None),
        P("dp", "block"),
    )
    out_specs = (
        P("dp", "block"),
        P("dp", "block"),
        P("block", "dp", None),
        P("block", "dp", None),
        P("block", "dp", None),
        P("block", "dp", None),
    )
    return jax.shard_map(local, mesh=mesh, in_specs=in_specs, out_specs=out_specs, check_vma=False)
```

```python
import functools

import jax
import jax.numpy as jnp
from jax import lax
from jax.experimental import pallas as pl
from jax.experimental.pallas import tpu as pltpu
from jax.sharding import PartitionSpec as P

ZL, CORES, NY, ZH, NX = 8, 2, 4, 2, 4
RING = ZL * ZH
BF = jnp.bfloat16
F32 = jnp.float32
PIECES = 2


def contract(form, left, right):
    return jnp.einsum(form, left, right, preferred_element_type=F32)


def place():
    dp = lax.axis_index("dp")
    block = lax.axis_index("block")
    zl, core = dp // CORES, dp % CORES
    y, rest = block // (ZH * NX), block % (ZH * NX)
    zh, x = rest // NX, rest % NX
    return zl, core, y, zh, x


def at(z, core, y, x):
    z = z % RING
    return {
        "dp": (z % ZL) * CORES + core,
        "block": y * (ZH * NX) + (z // ZL) * NX + x,
    }


def greet(others):
    barrier = pltpu.get_barrier_semaphore()
    for who in others:
        pl.semaphore_signal(barrier, inc=1, device_id=who, device_id_type=pl.DeviceIdType.MESH)
    pl.semaphore_wait(barrier, len(others))


def remote(src, dst, send, recv, target):
    return pltpu.make_async_remote_copy(
        src_ref=src,
        dst_ref=dst,
        send_sem=send,
        recv_sem=recv,
        device_id=target,
        device_id_type=pl.DeviceIdType.MESH,
    )


class Swap:
    STEPS = (3,)
    WAYS = (RING // 4, RING - RING // 4)

    @staticmethod
    def scratch(arrays):
        shape = arrays[0].shape
        return [
            pltpu.VMEM(shape, BF),
            pltpu.SemaphoreType.DMA((2, 2)),
            pltpu.SemaphoreType.DMA((2, 2)),
        ]

    @staticmethod
    def outs(arrays):
        return [jax.ShapeDtypeStruct(v.shape, v.dtype) for v in arrays]

    def __init__(self, ins, outs, scratch):
        self.src, self.out = ins[0], outs[0]
        self.relay, self.send, self.recv = scratch
        zl, core, y, zh, x = place()
        z = zh * ZL + zl
        self.targets = [at(z + way, core, y, x) for way in self.WAYS]

    def peers(self):
        return self.targets

    def start(self):
        self.first = [
            remote(
                self.src.at[j], self.relay.at[j], self.send.at[0, j], self.recv.at[0, j], who
            )
            for j, who in enumerate(self.targets)
        ]
        for copy in self.first:
            copy.start()

    def step(self, s):
        if s not in self.STEPS:
            return
        self.second = []
        for j, who in enumerate(self.targets):
            self.first[j].wait_recv()
            copy = remote(
                self.relay.at[j], self.out.at[j], self.send.at[1, j], self.recv.at[1, j], who
            )
            copy.start()
            self.second.append(copy)

    def finish(self):
        for copy in self.second:
            copy.wait_recv()
        for copy in self.first + self.second:
            copy.wait_send()


class Spread:
    RELAYS = (
        (0, 2, 0, 1),
        (2, 0, 1, 0),
        (3, 2, 0, 3),
        (2, 1, 3, 0),
        (1, 2, 0, 1),
        (2, 3, 3, 0),
        (2, 2, 0, 3),
    )
    STEPS = {1: (0, 1, 2), 2: (3, 4, 5, 6)}

    @staticmethod
    def scratch(arrays):
        n, hops = len(arrays), len(Spread.RELAYS)
        return [pltpu.VMEM((hops,) + v.shape[1:], BF) for v in arrays] + [
            pltpu.SemaphoreType.DMA((n, NY * NX)),
            pltpu.SemaphoreType.DMA((n, NY * NX)),
            pltpu.SemaphoreType.DMA((n, hops)),
            pltpu.SemaphoreType.DMA((n, hops)),
            pltpu.SemaphoreType.DMA((n,)),
        ]

    @staticmethod
    def outs(arrays):
        return [jax.ShapeDtypeStruct(v.shape, v.dtype) for v in arrays]

    def __init__(self, ins, outs, scratch):
        self.n = len(ins)
        self.src, self.out = ins, outs
        self.relay = scratch[: self.n]
        self.send, self.recv, self.rsend, self.rrecv, self.own = scratch[self.n :]
        zl, self.core, self.y, zh, self.x = place()
        self.z = zh * ZL + zl

    def device(self, dy, dx):
        return at(self.z, self.core, (self.y + dy) % NY, (self.x + dx) % NX)

    def index(self, dy, dx):
        return (self.y + dy) % NY * NX + (self.x + dx) % NX

    def peers(self):
        return [self.device(dy, dx) for dy in range(NY) for dx in range(NX) if dy or dx]

    def start(self):
        me = self.index(0, 0)
        self.sent, self.legs, self.keeps, self.comes = [], {}, [], []
        for j, (dy, dx, ry, rx) in enumerate(self.RELAYS):
            for w in range(self.n):
                copy = remote(
                    self.src[w].at[self.index(dy, dx)],
                    self.relay[w].at[j],
                    self.rsend.at[w, j],
                    self.rrecv.at[w, j],
                    self.device(ry, rx),
                )
                copy.start()
                self.legs[w, j] = copy
        for dy in range(NY):
            for dx in range(NX):
                if not (dy or dx) or 2 in (dy, dx):
                    continue
                for w in range(self.n):
                    copy = remote(
                        self.src[w].at[self.index(dy, dx)],
                        self.out[w].at[me],
                        self.send.at[w, dy * NX + dx],
                        self.recv.at[w, dy * NX + dx],
                        self.device(dy, dx),
                    )
                    copy.start()
                    self.sent.append(copy)
                    self.comes.append(copy)
        for w in range(self.n):
            keep = pltpu.make_async_copy(self.src[w].at[me], self.out[w].at[me], self.own.at[w])
            keep.start()
            self.keeps.append(keep)

    def step(self, s):
        for j in self.STEPS.get(s, ()):
            dy, dx, ry, rx = self.RELAYS[j]
            for w in range(self.n):
                self.legs[w, j].wait_recv()
                self.sent.append(self.legs[w, j])
                copy = remote(
                    self.relay[w].at[j],
                    self.out[w].at[self.index(NY - ry, NX - rx)],
                    self.send.at[w, dy * NX + dx],
                    self.recv.at[w, dy * NX + dx],
                    self.device(dy - ry + NY, dx - rx + NX),
                )
                copy.start()
                self.sent.append(copy)
                self.comes.append(copy)

    def finish(self):
        for copy in self.comes:
            copy.wait_recv()
        for copy in self.sent:
            copy.wait_send()
        for keep in self.keeps:
            keep.wait()


def halves(shapes):
    return [
        (w, pl.ds(i * (s[0] // PIECES), s[0] // PIECES))
        for w, s in enumerate(shapes)
        for i in range(PIECES)
    ]


def gather_kernel(count, kind, extra, *refs):
    own, refs = refs[:count], refs[count:]
    side_in, refs = refs[:extra], refs[extra:]
    out, refs = refs[:count], refs[count:]
    side_out, refs = refs[:extra], refs[extra:]
    (send, recv, local), refs = refs[:3], refs[3:]
    side = kind(side_in, side_out, refs)
    zl, core, y, zh, x = place()
    z = zh * ZL + zl
    right, left = at(z + 1, core, y, x), at(z + RING - 1, core, y, x)
    other = at(z, 1 - core, y, x)
    greet([right, left, other] + side.peers())

    pieces = halves([o.shape for o in own])
    total = range(len(pieces))

    def mine(p):
        w, part = pieces[p]
        return own[w].at[part]

    def spot(p, source):
        w, part = pieces[p]
        source = source % RING
        return out[w].at[source // ZL, part, source % ZL, core]

    def push(p, slot, source, target, src=None):
        where = spot(p, source)
        copy = remote(
            where if src is None else src, where, send.at[p, slot], recv.at[p, slot], target
        )
        copy.start()
        return copy

    half = RING // 2
    sent = []
    rights, lefts, keeps = [], [], []
    for p in total:
        rights.append(push(p, 0, z, right, mine(p)))
        lefts.append(push(p, half, z, left, mine(p)))
    side.start()
    for p in total:
        sent.append(push(p, RING - 1, z, other, mine(p)))
        keep = pltpu.make_async_copy(mine(p), spot(p, z), local.at[p])
        keep.start()
        keeps.append(keep)
    for s in range(1, half + 1):
        for p in total:
            rights[p].wait_recv()
            sent.append(rights[p])
            if s < half:
                rights[p] = push(p, s, z + RING - s, right)
            sent.append(push(p, RING + s, z + RING - s, other))
            if s < half:
                lefts[p].wait_recv()
                sent.append(lefts[p])
                if s < half - 1:
                    lefts[p] = push(p, half + s, z + s, left)
                sent.append(push(p, RING + half + s, z + s, other))
        side.step(s)
    side.finish()
    for p in total:
        for slot in [RING - 1] + list(range(RING + 1, 2 * RING)):
            remote(mine(p), mine(p), send.at[p, slot], recv.at[p, slot], other).wait_recv()
    for copy in sent:
        copy.wait_send()
    for keep in keeps:
        keep.wait()


def ring_gather(shards, kind, arrays, collective_id):
    count, extra = len(shards), len(arrays)
    slots = 2 * RING
    shapes = [
        jax.ShapeDtypeStruct((ZH, s.shape[0], ZL, CORES) + s.shape[1:], s.dtype) for s in shards
    ]
    outs = pl.pallas_call(
        functools.partial(gather_kernel, count, kind, extra),
        out_shape=shapes + kind.outs(arrays),
        in_specs=[pl.BlockSpec(memory_space=pltpu.VMEM)] * (count + extra),
        out_specs=[pl.BlockSpec(memory_space=pl.ANY)] * (count + extra),
        scratch_shapes=[
            pltpu.SemaphoreType.DMA((count * PIECES, slots)),
            pltpu.SemaphoreType.DMA((count * PIECES, slots)),
            pltpu.SemaphoreType.DMA((count * PIECES,)),
        ]
        + kind.scratch(arrays),
        compiler_params=pltpu.CompilerParams(
            collective_id=collective_id, has_side_effects=True, vmem_limit_bytes=10 * 2**20
        ),
        name="ring_gather",
    )(*shards, *arrays)
    full = [
        o.reshape(ZH * s.shape[0], ZL * CORES * s.shape[1], s.shape[2])
        for o, s in zip(outs[:count], shards)
    ]
    return full, outs[count:]


def scatter_kernel(count, kind, extra, *refs):
    part, refs = refs[:count], refs[count:]
    side_in, refs = refs[:extra], refs[extra:]
    out, refs = refs[:count], refs[count:]
    side_out, refs = refs[:extra], refs[extra:]
    mate, come, stage = refs[:count], refs[count : 2 * count], refs[2 * count : 3 * count]
    (send, recv, msend, mrecv), refs = refs[3 * count : 3 * count + 4], refs[3 * count + 4 :]
    side = kind(side_in, side_out, refs)
    zl, core, y, zh, x = place()
    z = zh * ZL + zl
    right, left = at(z + 1, core, y, x), at(z + RING - 1, core, y, x)
    other = at(z, 1 - core, y, x)
    greet([right, left, other] + side.peers())
    half = RING // 2

    def goal(slot):
        if slot < half:
            return (z + half - slot) % RING
        return (z + RING - (half - 1) + (slot - half)) % RING

    order = []
    for s in range(half):
        order.append(s)
        if half + s < RING - 1:
            order.append(half + s)
    order.append(RING - 1)

    pieces = halves([o.shape for o in out])
    mates = {}

    def trade(slot):
        d = goal(slot)
        for p, (w, rows) in enumerate(pieces):
            copy = remote(
                part[w].at[d // ZL, rows, d % ZL, 1 - core],
                mate[w].at[slot, rows],
                msend.at[p, slot],
                mrecv.at[p, slot],
                other,
            )
            copy.start()
            mates[p, slot] = copy

    for slot in order[:4]:
        trade(slot)
    side.start()
    for slot in order[4:]:
        trade(slot)
    moves = {}
    for slot in order:
        d = goal(slot)
        for p, (w, rows) in enumerate(pieces):
            mates[p, slot].wait_recv()
            total = part[w][d // ZL, rows, d % ZL, core].astype(F32)
            total = total + mate[w][slot, rows].astype(F32)
            if slot == RING - 1:
                for last in (half - 1, RING - 2):
                    moves[p, last].wait_recv()
                    total = total + come[w][last, rows].astype(F32)
                out[w][rows] = total
                continue
            if slot not in (0, half):
                moves[p, slot - 1].wait_recv()
                total = total + come[w][slot - 1, rows].astype(F32)
            stage[w][slot, rows] = total.astype(BF)
            copy = remote(
                stage[w].at[slot, rows],
                come[w].at[slot, rows],
                send.at[p, slot],
                recv.at[p, slot],
                right if slot < half else left,
            )
            copy.start()
            moves[p, slot] = copy
        if slot < half:
            side.step(slot)
    side.finish()
    for copy in mates.values():
        copy.wait_send()
    for copy in moves.values():
        copy.wait_send()


def ring_scatter(parts, kind, arrays, collective_id):
    count, extra = len(parts), len(arrays)
    split, shards = [], []
    for p in parts:
        shard = (p.shape[0] // ZH, p.shape[1] // (ZL * CORES), p.shape[2])
        shards.append(shard)
        split.append(p.reshape(ZH, shard[0], ZL, CORES, shard[1], shard[2]))
    outs = pl.pallas_call(
        functools.partial(scatter_kernel, count, kind, extra),
        out_shape=[jax.ShapeDtypeStruct(s, F32) for s in shards] + kind.outs(arrays),
        in_specs=[pl.BlockSpec(memory_space=pltpu.VMEM)] * (count + extra),
        out_specs=[pl.BlockSpec(memory_space=pltpu.VMEM)] * count
        + [pl.BlockSpec(memory_space=pl.ANY)] * extra,
        scratch_shapes=[pltpu.VMEM((RING,) + s, BF) for s in shards]
        + [pltpu.VMEM((RING - 1,) + s, BF) for s in shards]
        + [pltpu.VMEM((RING - 1,) + s, BF) for s in shards]
        + [
            pltpu.SemaphoreType.DMA((count * PIECES, RING - 1)),
            pltpu.SemaphoreType.DMA((count * PIECES, RING - 1)),
            pltpu.SemaphoreType.DMA((count * PIECES, RING)),
            pltpu.SemaphoreType.DMA((count * PIECES, RING)),
        ]
        + kind.scratch(arrays),
        compiler_params=pltpu.CompilerParams(
            collective_id=collective_id, has_side_effects=True, vmem_limit_bytes=48 * 2**20
        ),
        name="ring_scatter",
    )(*split, *arrays)
    return outs[:count], outs[count:]


def columns_out(v):
    k, e, c, t = v.shape
    cols = c // (NY * ZH * NX)
    v = v.reshape(k * e, NY, ZH, NX, cols, t).transpose(1, 3, 2, 4, 0, 5)
    return v.reshape(NY * NX, ZH * cols, k * e, t)


def columns_in(v):
    peers, c, a, t = v.shape
    v = v.reshape(NY, NX, c, ZH, a // ZH, t).transpose(2, 0, 3, 1, 4, 5)
    return v.reshape(c, peers * a, t)


def rows_out(v):
    c, a, t = v.shape
    rows = a // (NY * ZH * NX)
    v = v.reshape(c, NY, ZH, NX, rows, t).transpose(1, 3, 2, 4, 0, 5)
    return v.reshape(NY * NX, ZH * rows, c, t)


def rows_in(v, k):
    peers, a, c, t = v.shape
    v = v.reshape(NY, NX, a, ZH, c // ZH, t).transpose(2, 0, 3, 1, 4, 5)
    return v.reshape(k, a // k * peers * c, t)


def local(tokens, upper_left, upper_right, lower_right, lower_left, cotangent):
    zl, core, y, zh, x = place()
    rows, features = tokens.shape
    width = upper_left.shape[1] * ZL * CORES
    kl = upper_left.shape[0]
    k4 = ZH * kl
    expand = upper_left.shape[2] // width
    few = rows // ZH
    low = zh == 0

    both = jnp.stack([tokens, cotangent]).reshape(2, ZH, few, kl, width).transpose(0, 1, 3, 2, 4)
    mine = jnp.where(low, both[:, 0], both[:, 1])
    away = jnp.where(low, both[:, 1], both[:, 0])
    (in_left, out_left), (came,) = ring_gather((upper_left, lower_left), Swap, (away,), 1)
    pair = jnp.concatenate(
        [jnp.where(low, mine, came), jnp.where(low, came, mine)], axis=1
    )
    toks, cots = pair[0], pair[1]

    mixed = contract("ktb,kbj->kjt", toks, in_left).astype(BF)
    back_narrow = contract("kto,kjo->kjt", cots, out_left).astype(BF)
    (in_right, out_right), (spread, narrow_back) = ring_gather(
        (upper_right, lower_right),
        Spread,
        (
            columns_out(mixed.reshape(k4, expand, width, few)),
            columns_out(back_narrow.reshape(k4, expand, width, few)),
        ),
        2,
    )
    spread, narrow_back = columns_in(spread), columns_in(narrow_back)

    hidden_pre = contract("cat,cab->cbt", spread, in_right)
    active = jax.nn.gelu(hidden_pre).astype(BF)
    narrow = contract("cbt,cbe->cet", active, out_right).astype(BF)
    back_active = contract("cet,cbe->cbt", narrow_back, out_right)
    back_pre = jax.vjp(jax.nn.gelu, hidden_pre)[1](back_active)[0].astype(BF)
    back_mixed = contract("cbt,cab->cat", back_pre, in_right).astype(BF)
    grad_lower_right = contract("cbt,cet->cbe", active, narrow_back).astype(BF)
    grad_upper_right = contract("cat,cbt->cab", spread, back_pre).astype(BF)
    (g_ur, g_lr), (narrow, back_mixed) = ring_scatter(
        (grad_upper_right, grad_lower_right), Spread, (rows_out(narrow), rows_out(back_mixed)), 3
    )
    narrow, back_mixed = rows_in(narrow, k4), rows_in(back_mixed, k4)

    result = contract("kjt,kjo->kto", narrow, out_left).astype(BF)
    token_grad = contract("kjt,kbj->ktb", back_mixed, in_left).astype(BF)
    grad_lower_left = contract("kjt,kto->kjo", narrow, cots).astype(BF)
    grad_upper_left = contract("ktb,kjt->kbj", toks, back_mixed).astype(BF)

    ends = jnp.stack([result, token_grad]).reshape(2, ZH, kl, few, width)
    keep = jnp.where(low, ends[:, 0], ends[:, 1])
    away = jnp.where(low, ends[:, 1], ends[:, 0])
    (g_ul, g_ll), (came,) = ring_scatter((grad_upper_left, grad_lower_left), Swap, (away,), 4)
    ends = jnp.stack([jnp.where(low, keep, came), jnp.where(low, came, keep)], axis=1)
    ends = ends.transpose(0, 1, 3, 2, 4).reshape(2, rows, features)
    return ends[0], ends[1], g_ul, g_ur, g_lr, g_ll


def solution(mesh):
    in_specs = (
        P("dp", "block"),
        P("block", "dp", None),
        P("block", "dp", None),
        P("block", "dp", None),
        P("block", "dp", None),
        P("dp", "block"),
    )
    out_specs = (
        P("dp", "block"),
        P("dp", "block"),
        P("block", "dp", None),
        P("block", "dp", None),
        P("block", "dp", None),
        P("block", "dp", None),
    )
    return jax.shard_map(local, mesh=mesh, in_specs=in_specs, out_specs=out_specs, check_vma=False)
```

```python
import functools

import jax
import jax.numpy as jnp
from jax import lax
from jax.experimental import pallas as pl
from jax.experimental.pallas import tpu as pltpu
from jax.sharding import PartitionSpec as P

ZL, CORES, NY, ZH, NX = 8, 2, 4, 2, 4
RING = ZL * ZH
BF = jnp.bfloat16
F32 = jnp.float32
PIECES = 2


def contract(form, left, right):
    return jnp.einsum(form, left, right, preferred_element_type=F32)


def place():
    dp = lax.axis_index("dp")
    block = lax.axis_index("block")
    zl, core = dp // CORES, dp % CORES
    y, rest = block // (ZH * NX), block % (ZH * NX)
    zh, x = rest // NX, rest % NX
    return zl, core, y, zh, x


def at(z, core, y, x):
    z = z % RING
    return {
        "dp": (z % ZL) * CORES + core,
        "block": y * (ZH * NX) + (z // ZL) * NX + x,
    }


def greet(others):
    barrier = pltpu.get_barrier_semaphore()
    for who in others:
        pl.semaphore_signal(barrier, inc=1, device_id=who, device_id_type=pl.DeviceIdType.MESH)
    pl.semaphore_wait(barrier, len(others))


def remote(src, dst, send, recv, target):
    return pltpu.make_async_remote_copy(
        src_ref=src,
        dst_ref=dst,
        send_sem=send,
        recv_sem=recv,
        device_id=target,
        device_id_type=pl.DeviceIdType.MESH,
    )


class Swap:
    CUTS, LAG = 4, 3
    WAYS = (RING // 4, RING - RING // 4)

    @staticmethod
    def scratch(arrays):
        shape = arrays[0].shape
        return [
            pltpu.VMEM(shape, BF),
            pltpu.SemaphoreType.DMA((2, 2, Swap.CUTS)),
            pltpu.SemaphoreType.DMA((2, 2, Swap.CUTS)),
        ]

    @staticmethod
    def outs(arrays):
        return [jax.ShapeDtypeStruct(v.shape, v.dtype) for v in arrays]

    def __init__(self, ins, outs, scratch):
        self.src, self.out = ins[0], outs[0]
        self.relay, self.send, self.recv = scratch
        zl, core, y, zh, x = place()
        z = zh * ZL + zl
        self.targets = [at(z + way, core, y, x) for way in self.WAYS]

    def peers(self):
        return self.targets

    def cut(self, j, i):
        kl, few = self.src.shape[1:3]
        per = self.CUTS // kl
        return j, i // per, pl.ds(i % per * (few // per), few // per)

    def leg(self, src, dst, number, i):
        copies = []
        for j, who in enumerate(self.targets):
            spot = self.cut(j, i)
            copy = remote(
                src.at[spot], dst.at[spot], self.send.at[number, j, i], self.recv.at[number, j, i], who
            )
            copy.start()
            copies.append(copy)
        return copies

    def start(self):
        self.first = [self.leg(self.src, self.relay, 0, 0)]
        self.second = []

    def step(self, s):
        if 1 <= s < self.CUTS:
            self.first.append(self.leg(self.src, self.relay, 0, s))
        if self.LAG <= s < self.LAG + self.CUTS:
            for copy in self.first[s - self.LAG]:
                copy.wait_recv()
            self.second.append(self.leg(self.relay, self.out, 1, s - self.LAG))

    def finish(self):
        for copies in self.second:
            for copy in copies:
                copy.wait_recv()
        for copies in self.first + self.second:
            for copy in copies:
                copy.wait_send()


class Spread:
    RELAYS = (
        (0, 2, 0, 1),
        (2, 0, 1, 0),
        (3, 2, 0, 3),
        (2, 1, 3, 0),
        (1, 2, 0, 1),
        (2, 3, 3, 0),
        (2, 2, 0, 3),
    )
    STEPS = {1: (0, 1, 2), 2: (3, 4, 5, 6)}

    @staticmethod
    def scratch(arrays):
        n, hops = len(arrays), len(Spread.RELAYS)
        return [pltpu.VMEM((hops,) + v.shape[1:], BF) for v in arrays] + [
            pltpu.SemaphoreType.DMA((n, NY * NX)),
            pltpu.SemaphoreType.DMA((n, NY * NX)),
            pltpu.SemaphoreType.DMA((n, hops)),
            pltpu.SemaphoreType.DMA((n, hops)),
            pltpu.SemaphoreType.DMA((n,)),
        ]

    @staticmethod
    def outs(arrays):
        return [jax.ShapeDtypeStruct(v.shape, v.dtype) for v in arrays]

    def __init__(self, ins, outs, scratch):
        self.n = len(ins)
        self.src, self.out = ins, outs
        self.relay = scratch[: self.n]
        self.send, self.recv, self.rsend, self.rrecv, self.own = scratch[self.n :]
        zl, self.core, self.y, zh, self.x = place()
        self.z = zh * ZL + zl

    def device(self, dy, dx):
        return at(self.z, self.core, (self.y + dy) % NY, (self.x + dx) % NX)

    def route(self, j, w):
        dy, dx, ry, rx = self.RELAYS[j]
        return (dx, dy, rx, ry) if w % 2 else (dy, dx, ry, rx)

    def index(self, dy, dx):
        return (self.y + dy) % NY * NX + (self.x + dx) % NX

    def peers(self):
        return [self.device(dy, dx) for dy in range(NY) for dx in range(NX) if dy or dx]

    def start(self):
        me = self.index(0, 0)
        self.sent, self.legs, self.keeps, self.comes = [], {}, [], []
        for j in range(len(self.RELAYS)):
            for w in range(self.n):
                dy, dx, ry, rx = self.route(j, w)
                copy = remote(
                    self.src[w].at[self.index(dy, dx)],
                    self.relay[w].at[j],
                    self.rsend.at[w, j],
                    self.rrecv.at[w, j],
                    self.device(ry, rx),
                )
                copy.start()
                self.legs[w, j] = copy
        for dy in range(NY):
            for dx in range(NX):
                if not (dy or dx) or 2 in (dy, dx):
                    continue
                for w in range(self.n):
                    copy = remote(
                        self.src[w].at[self.index(dy, dx)],
                        self.out[w].at[me],
                        self.send.at[w, dy * NX + dx],
                        self.recv.at[w, dy * NX + dx],
                        self.device(dy, dx),
                    )
                    copy.start()
                    self.sent.append(copy)
                    self.comes.append(copy)
        for w in range(self.n):
            keep = pltpu.make_async_copy(self.src[w].at[me], self.out[w].at[me], self.own.at[w])
            keep.start()
            self.keeps.append(keep)

    def step(self, s):
        for j in self.STEPS.get(s, ()):
            for w in range(self.n):
                dy, dx, ry, rx = self.route(j, w)
                self.legs[w, j].wait_recv()
                self.sent.append(self.legs[w, j])
                copy = remote(
                    self.relay[w].at[j],
                    self.out[w].at[self.index(NY - ry, NX - rx)],
                    self.send.at[w, dy * NX + dx],
                    self.recv.at[w, dy * NX + dx],
                    self.device(dy - ry + NY, dx - rx + NX),
                )
                copy.start()
                self.sent.append(copy)
                self.comes.append(copy)

    def finish(self):
        for copy in self.comes:
            copy.wait_recv()
        for copy in self.sent:
            copy.wait_send()
        for keep in self.keeps:
            keep.wait()


def halves(shapes):
    return [
        (w, pl.ds(i * (s[0] // PIECES), s[0] // PIECES))
        for w, s in enumerate(shapes)
        for i in range(PIECES)
    ]


def gather_kernel(count, kind, extra, *refs):
    own, refs = refs[:count], refs[count:]
    side_in, refs = refs[:extra], refs[extra:]
    out, refs = refs[:count], refs[count:]
    side_out, refs = refs[:extra], refs[extra:]
    (send, recv, local), refs = refs[:3], refs[3:]
    side = kind(side_in, side_out, refs)
    zl, core, y, zh, x = place()
    z = zh * ZL + zl
    right, left = at(z + 1, core, y, x), at(z + RING - 1, core, y, x)
    other = at(z, 1 - core, y, x)
    greet([right, left, other] + side.peers())

    pieces = halves([o.shape for o in own])
    total = range(len(pieces))

    def mine(p):
        w, part = pieces[p]
        return own[w].at[part]

    def spot(p, source):
        w, part = pieces[p]
        source = source % RING
        return out[w].at[source // ZL, part, source % ZL, core]

    def push(p, slot, source, target, src=None):
        where = spot(p, source)
        copy = remote(
            where if src is None else src, where, send.at[p, slot], recv.at[p, slot], target
        )
        copy.start()
        return copy

    half = RING // 2
    sent = []
    rights, lefts, keeps = [], [], []
    for p in total:
        rights.append(push(p, 0, z, right, mine(p)))
        lefts.append(push(p, half, z, left, mine(p)))
    side.start()
    for p in total:
        sent.append(push(p, RING - 1, z, other, mine(p)))
        keep = pltpu.make_async_copy(mine(p), spot(p, z), local.at[p])
        keep.start()
        keeps.append(keep)
    for s in range(1, half + 1):
        for p in total:
            rights[p].wait_recv()
            sent.append(rights[p])
            if s < half:
                rights[p] = push(p, s, z + RING - s, right)
            sent.append(push(p, RING + s, z + RING - s, other))
            if s < half:
                lefts[p].wait_recv()
                sent.append(lefts[p])
                if s < half - 1:
                    lefts[p] = push(p, half + s, z + s, left)
                sent.append(push(p, RING + half + s, z + s, other))
        side.step(s)
    side.finish()
    for p in total:
        for slot in [RING - 1] + list(range(RING + 1, 2 * RING)):
            remote(mine(p), mine(p), send.at[p, slot], recv.at[p, slot], other).wait_recv()
    for copy in sent:
        copy.wait_send()
    for keep in keeps:
        keep.wait()


def ring_gather(shards, kind, arrays, collective_id):
    count, extra = len(shards), len(arrays)
    slots = 2 * RING
    shapes = [
        jax.ShapeDtypeStruct((ZH, s.shape[0], ZL, CORES) + s.shape[1:], s.dtype) for s in shards
    ]
    outs = pl.pallas_call(
        functools.partial(gather_kernel, count, kind, extra),
        out_shape=shapes + kind.outs(arrays),
        in_specs=[pl.BlockSpec(memory_space=pltpu.VMEM)] * (count + extra),
        out_specs=[pl.BlockSpec(memory_space=pl.ANY)] * (count + extra),
        scratch_shapes=[
            pltpu.SemaphoreType.DMA((count * PIECES, slots)),
            pltpu.SemaphoreType.DMA((count * PIECES, slots)),
            pltpu.SemaphoreType.DMA((count * PIECES,)),
        ]
        + kind.scratch(arrays),
        compiler_params=pltpu.CompilerParams(
            collective_id=collective_id, has_side_effects=True, vmem_limit_bytes=10 * 2**20
        ),
        name="ring_gather",
    )(*shards, *arrays)
    full = [
        o.reshape(ZH * s.shape[0], ZL * CORES * s.shape[1], s.shape[2])
        for o, s in zip(outs[:count], shards)
    ]
    return full, outs[count:]


def scatter_kernel(count, kind, extra, *refs):
    part, refs = refs[:count], refs[count:]
    side_in, refs = refs[:extra], refs[extra:]
    out, refs = refs[:count], refs[count:]
    side_out, refs = refs[:extra], refs[extra:]
    mate, come, stage = refs[:count], refs[count : 2 * count], refs[2 * count : 3 * count]
    (send, recv, msend, mrecv), refs = refs[3 * count : 3 * count + 4], refs[3 * count + 4 :]
    side = kind(side_in, side_out, refs)
    zl, core, y, zh, x = place()
    z = zh * ZL + zl
    right, left = at(z + 1, core, y, x), at(z + RING - 1, core, y, x)
    other = at(z, 1 - core, y, x)
    greet([right, left, other] + side.peers())
    half = RING // 2

    def goal(slot):
        if slot < half:
            return (z + half - slot) % RING
        return (z + RING - (half - 1) + (slot - half)) % RING

    order = []
    for s in range(half):
        order.append(s)
        if half + s < RING - 1:
            order.append(half + s)
    order.append(RING - 1)

    pieces = halves([o.shape for o in out])
    mates = {}

    def trade(slot):
        d = goal(slot)
        for p, (w, rows) in enumerate(pieces):
            copy = remote(
                part[w].at[d // ZL, rows, d % ZL, 1 - core],
                mate[w].at[slot, rows],
                msend.at[p, slot],
                mrecv.at[p, slot],
                other,
            )
            copy.start()
            mates[p, slot] = copy

    for slot in order[:4]:
        trade(slot)
    side.start()
    for slot in order[4:]:
        trade(slot)
    moves = {}
    for slot in order:
        d = goal(slot)
        for p, (w, rows) in enumerate(pieces):
            mates[p, slot].wait_recv()
            total = part[w][d // ZL, rows, d % ZL, core].astype(F32)
            total = total + mate[w][slot, rows].astype(F32)
            if slot == RING - 1:
                for last in (half - 1, RING - 2):
                    moves[p, last].wait_recv()
                    total = total + come[w][last, rows].astype(F32)
                out[w][rows] = total
                continue
            if slot not in (0, half):
                moves[p, slot - 1].wait_recv()
                total = total + come[w][slot - 1, rows].astype(F32)
            stage[w][slot, rows] = total.astype(BF)
            copy = remote(
                stage[w].at[slot, rows],
                come[w].at[slot, rows],
                send.at[p, slot],
                recv.at[p, slot],
                right if slot < half else left,
            )
            copy.start()
            moves[p, slot] = copy
        if slot < half:
            side.step(slot)
    side.finish()
    for copy in mates.values():
        copy.wait_send()
    for copy in moves.values():
        copy.wait_send()


def ring_scatter(parts, kind, arrays, collective_id):
    count, extra = len(parts), len(arrays)
    split, shards = [], []
    for p in parts:
        shard = (p.shape[0] // ZH, p.shape[1] // (ZL * CORES), p.shape[2])
        shards.append(shard)
        split.append(p.reshape(ZH, shard[0], ZL, CORES, shard[1], shard[2]))
    outs = pl.pallas_call(
        functools.partial(scatter_kernel, count, kind, extra),
        out_shape=[jax.ShapeDtypeStruct(s, F32) for s in shards] + kind.outs(arrays),
        in_specs=[pl.BlockSpec(memory_space=pltpu.VMEM)] * (count + extra),
        out_specs=[pl.BlockSpec(memory_space=pltpu.VMEM)] * count
        + [pl.BlockSpec(memory_space=pl.ANY)] * extra,
        scratch_shapes=[pltpu.VMEM((RING,) + s, BF) for s in shards]
        + [pltpu.VMEM((RING - 1,) + s, BF) for s in shards]
        + [pltpu.VMEM((RING - 1,) + s, BF) for s in shards]
        + [
            pltpu.SemaphoreType.DMA((count * PIECES, RING - 1)),
            pltpu.SemaphoreType.DMA((count * PIECES, RING - 1)),
            pltpu.SemaphoreType.DMA((count * PIECES, RING)),
            pltpu.SemaphoreType.DMA((count * PIECES, RING)),
        ]
        + kind.scratch(arrays),
        compiler_params=pltpu.CompilerParams(
            collective_id=collective_id, has_side_effects=True, vmem_limit_bytes=48 * 2**20
        ),
        name="ring_scatter",
    )(*split, *arrays)
    return outs[:count], outs[count:]


def columns_out(v):
    k, e, c, t = v.shape
    cols = c // (NY * ZH * NX)
    v = v.reshape(k * e, NY, ZH, NX, cols, t).transpose(1, 3, 2, 4, 0, 5)
    return v.reshape(NY * NX, ZH * cols, k * e, t)


def columns_in(v):
    peers, c, a, t = v.shape
    v = v.reshape(NY, NX, c, ZH, a // ZH, t).transpose(2, 0, 3, 1, 4, 5)
    return v.reshape(c, peers * a, t)


def rows_out(v):
    c, a, t = v.shape
    rows = a // (NY * ZH * NX)
    v = v.reshape(c, NY, ZH, NX, rows, t).transpose(1, 3, 2, 4, 0, 5)
    return v.reshape(NY * NX, ZH * rows, c, t)


def rows_in(v, k):
    peers, a, c, t = v.shape
    v = v.reshape(NY, NX, a, ZH, c // ZH, t).transpose(2, 0, 3, 1, 4, 5)
    return v.reshape(k, a // k * peers * c, t)


def local(tokens, upper_left, upper_right, lower_right, lower_left, cotangent):
    zl, core, y, zh, x = place()
    rows, features = tokens.shape
    width = upper_left.shape[1] * ZL * CORES
    kl = upper_left.shape[0]
    k4 = ZH * kl
    expand = upper_left.shape[2] // width
    few = rows // ZH
    low = zh == 0

    both = jnp.stack([tokens, cotangent]).reshape(2, ZH, few, kl, width).transpose(0, 1, 3, 2, 4)
    mine = jnp.where(low, both[:, 0], both[:, 1])
    away = jnp.where(low, both[:, 1], both[:, 0])
    (in_left, out_left), (came,) = ring_gather((upper_left, lower_left), Swap, (away,), 1)
    pair = jnp.concatenate(
        [jnp.where(low, mine, came), jnp.where(low, came, mine)], axis=1
    )
    toks, cots = pair[0], pair[1]

    mixed = contract("ktb,kbj->kjt", toks, in_left).astype(BF)
    back_narrow = contract("kto,kjo->kjt", cots, out_left).astype(BF)
    (in_right, out_right), (spread, narrow_back) = ring_gather(
        (upper_right, lower_right),
        Spread,
        (
            columns_out(mixed.reshape(k4, expand, width, few)),
            columns_out(back_narrow.reshape(k4, expand, width, few)),
        ),
        2,
    )
    spread, narrow_back = columns_in(spread), columns_in(narrow_back)

    hidden_pre = contract("cat,cab->cbt", spread, in_right)
    active = jax.nn.gelu(hidden_pre).astype(BF)
    narrow = contract("cbt,cbe->cet", active, out_right).astype(BF)
    back_active = contract("cet,cbe->cbt", narrow_back, out_right)
    back_pre = jax.vjp(jax.nn.gelu, hidden_pre)[1](back_active)[0].astype(BF)
    back_mixed = contract("cbt,cab->cat", back_pre, in_right).astype(BF)
    grad_lower_right = contract("cbt,cet->cbe", active, narrow_back).astype(BF)
    grad_upper_right = contract("cat,cbt->cab", spread, back_pre).astype(BF)
    (g_ur, g_lr), (narrow, back_mixed) = ring_scatter(
        (grad_upper_right, grad_lower_right), Spread, (rows_out(narrow), rows_out(back_mixed)), 3
    )
    narrow, back_mixed = rows_in(narrow, k4), rows_in(back_mixed, k4)

    result = contract("kjt,kjo->kto", narrow, out_left).astype(BF)
    token_grad = contract("kjt,kbj->ktb", back_mixed, in_left).astype(BF)
    grad_lower_left = contract("kjt,kto->kjo", narrow, cots).astype(BF)
    grad_upper_left = contract("ktb,kjt->kbj", toks, back_mixed).astype(BF)

    ends = jnp.stack([result, token_grad]).reshape(2, ZH, kl, few, width)
    keep = jnp.where(low, ends[:, 0], ends[:, 1])
    away = jnp.where(low, ends[:, 1], ends[:, 0])
    (g_ul, g_ll), (came,) = ring_scatter((grad_upper_left, grad_lower_left), Swap, (away,), 4)
    ends = jnp.stack([jnp.where(low, keep, came), jnp.where(low, came, keep)], axis=1)
    ends = ends.transpose(0, 1, 3, 2, 4).reshape(2, rows, features)
    return ends[0], ends[1], g_ul, g_ur, g_lr, g_ll


def solution(mesh):
    in_specs = (
        P("dp", "block"),
        P("block", "dp", None),
        P("block", "dp", None),
        P("block", "dp", None),
        P("block", "dp", None),
        P("dp", "block"),
    )
    out_specs = (
        P("dp", "block"),
        P("dp", "block"),
        P("block", "dp", None),
        P("block", "dp", None),
        P("block", "dp", None),
        P("block", "dp", None),
    )
    return jax.shard_map(local, mesh=mesh, in_specs=in_specs, out_specs=out_specs, check_vma=False)
```
